32 devices in a mesh: ep: 16 (over z, y, x), dp: 2 (over core).
Axes of the slice: x: 2, y: 2, z: 4, core: 2. Of those that a mesh axis runs over, the one named last changes fastest.
Arguments:
- layer_input: bfloat16 [2048, 3584], P('ep'), may hold values from -6 to 6
- out_grad: bfloat16 [2048, 3584], P('ep'), may hold values from -6 to 6
- expert_ids: int32 [2048, 8], P('ep'), may hold values from 0 to 15, all different within a row; in each aligned block of 128 rows (0 to 127, 128 to 255, ...) at most 80 rows name the same one
- gate_probs: float32 [2048, 8], P('ep'), may hold values from 0.1 to 1
- gate_proj: bfloat16 [16, 3584, 1024], P('ep'), may hold values from -0.09375 to 0.09375
- up_proj: bfloat16 [16, 3584, 1024], P('ep'), may hold values from -0.09375 to 0.09375
- down_proj: bfloat16 [16, 1024, 3584], P('ep'), may hold values from -0.1875 to 0.1875
Outputs:
- input_grad: bfloat16 [2048, 3584], P('ep', 'dp')
The draws below stay inside these ranges and needn't reach their ends.
Inputs may be any that keep to these rules, and one draw needn't show every extreme that they name: `expert_ids`: each row names 8 different experts. The 128 rows of one device name one expert at most 80 times, and in every draw some device's rows name some expert exactly 80 times.
All inputs are finite; a program needn't handle non-finite values.
Results may differ from the reference program's by a relative error of at most 0.0058.
Values may be sent and summed in bfloat16 or wider, within the bound.
A program may use at most 192 MiB of HBM per device.

```python
import math
import jax
import jax.numpy as jnp
import numpy as np
from jax import lax

D = 3584
FF = 1024
TOP = 8
TOK_DEV = 128
EXPERTS = 16
CAP = 80
TOKENS = 2048
N_EP = 16


def level_of(rng, extent, shards, least, high):
    gain, own = 1.0, jax.random.fold_in(rng, 6)
    for dim, parts in shards:
        heights = jnp.exp(jax.random.uniform(jax.random.fold_in(own, dim), (parts,), jnp.float32, least / len(shards), high / len(shards)))
        gain = gain * jnp.repeat(heights, extent[dim] // parts).reshape([-1 if axis == dim else 1 for axis in range(len(extent))])
    return gain


def assign_block(rng, own, number, rows, amount, top, limit, lean):
    order = jax.random.permutation(rng, amount)
    packed, usual = portions_of(amount, rows * top, limit, lean, True), portions_of(amount, rows * top, limit, lean, False)
    places = jnp.arange(amount)

    def named(sizes, turn):
        used = int((sizes > 0).sum())
        fixed = max(1, used // 4)
        moved = fixed + (places - fixed + turn * (used - fixed)) % max(1, amount - fixed)
        return jnp.zeros((amount,), jnp.int32).at[order[jnp.where(places < fixed, places, moved)]].set(jnp.asarray(sizes, jnp.int32))

    sizes = jnp.where(number % 4 == 0, named(packed, number // 4), named(usual, number - number // 4 - 1))
    mixed = jax.random.permutation(jax.random.fold_in(own, 3), amount)
    donor, sink = mixed[0:amount // 2 * 2:2], mixed[1:amount // 2 * 2:2]
    room = jnp.minimum(sizes[donor] - 1, limit - sizes[sink]) // 2
    room = jnp.where((donor == order[0]) | (sink == order[0]) | (sizes[sink] == 0), 0, jnp.maximum(room, 0))
    moved = jax.random.randint(jax.random.fold_in(own, 4), (amount // 2,), 0, 1 << 20) % (room + 1)
    sizes = sizes.at[donor].add(-moved).at[sink].add(moved)
    labels = jnp.searchsorted(jnp.cumsum(sizes), jnp.arange(rows * top), side="right").astype(jnp.int32)
    listing = labels.reshape(top, rows).T
    listing = listing[jax.random.permutation(jax.random.fold_in(own, 1), rows)]
    turn = jax.random.randint(jax.random.fold_in(own, 2), (rows, 1), 0, top)
    return jnp.take_along_axis(listing, (jnp.arange(top)[None, :] + turn) % top, axis=1)


def portions_of(number_of, total, reach, slope, full):
    weights = [(1 << 20) // math.isqrt(rank ** slope) + 1 for rank in range(1, number_of + 1)]
    largest = reach if full else min(reach, max(-(-total // number_of), total * weights[0] // sum(weights)))
    least = 1 if total - largest >= number_of - 1 else 0
    given, surplus = [largest] + [least] * (number_of - 1), total - largest - least * (number_of - 1)
    while surplus > 0:
        movable = [i for i in range(1, number_of) if given[i] < largest] or [i for i in range(1, number_of) if given[i] < reach]
        whole, budget = sum([weights[i] for i in movable]), surplus
        for i in movable:
            extra = min(reach - given[i], max(1, budget * weights[i] // whole), surplus)
            given[i] = given[i] + extra
            surplus = surplus - extra
    return np.array(given)


def bell_draw(stream_key, extent, deviation, most, pieces=(), kind=jnp.bfloat16):
    drawn = jax.random.normal(stream_key, extent, jnp.float32) * deviation
    if len(pieces) > 0:
        drawn = level_of(stream_key, extent, pieces, -0.22, 0.18) * drawn
    return jnp.clip(drawn, min=-most, max=most).astype(kind)


def setup_inputs(seed: int = 0) -> dict:
    streams_of = jax.random.split(jax.random.key(seed), 8)
    layer_input = bell_draw(streams_of[0], (TOKENS, D), 1.0, 6.0, ((0, 16),))
    out_grad = bell_draw(streams_of[1], (TOKENS, D), 1.0, 6.0, ((0, 16),))
    expert_ids_keys = jax.random.split(jax.random.fold_in(streams_of[2], 1), TOKENS // TOK_DEV)
    expert_ids_turns = jax.random.permutation(jax.random.fold_in(streams_of[2], 3), TOKENS // TOK_DEV)
    expert_ids = jax.vmap(lambda own, number: assign_block(jax.random.fold_in(streams_of[2], 2), own, number, TOK_DEV, EXPERTS, TOP, CAP, 1))(expert_ids_keys, expert_ids_turns).reshape((TOKENS, TOP))
    gate_probs = jnp.clip(0.1 + 0.9 * jax.random.uniform(streams_of[3], (TOKENS, TOP), jnp.float32) ** level_of(streams_of[3], (TOKENS, TOP), ((0, 16),), -0.2, 0.2), 0.1, 1.0)
    gate_proj = bell_draw(streams_of[4], (EXPERTS, D, FF), D ** -0.5, 0.09375, ((0, 16),))
    up_proj = bell_draw(streams_of[5], (EXPERTS, D, FF), D ** -0.5, 0.09375, ((0, 16),))
    down_proj = bell_draw(streams_of[6], (EXPERTS, FF, D), FF ** -0.5, 0.1875, ((0, 16),))
    return {"layer_input": layer_input, "out_grad": out_grad, "expert_ids": expert_ids, "gate_probs": gate_probs, "gate_proj": gate_proj, "up_proj": up_proj, "down_proj": down_proj}


def slot_ranks(flat_ids, experts_count):
    onehot = (flat_ids[:, None] == jnp.arange(experts_count, dtype=jnp.int32)[None, :]).astype(jnp.int32)
    running = jnp.cumsum(onehot, axis=0)
    return jnp.sum((running - 1) * onehot, axis=1).astype(jnp.int32)


def expert_backward(in_rows, grad_rows, gate_mat, up_mat, down_mat):
    gate_pre = jnp.dot(in_rows, gate_mat, preferred_element_type=jnp.float32)
    up_pre = jnp.dot(in_rows, up_mat, preferred_element_type=jnp.float32)
    hidden_grad = lax.dot_general(grad_rows, down_mat, (((1,), (1,)), ((), ())), preferred_element_type=jnp.float32)
    sigmoid = jax.nn.sigmoid(gate_pre)
    gate_grad = (hidden_grad * up_pre * sigmoid * (1.0 + gate_pre * (1.0 - sigmoid))).astype(jnp.bfloat16)
    up_grad = (hidden_grad * gate_pre * sigmoid).astype(jnp.bfloat16)
    back_gate = lax.dot_general(gate_grad, gate_mat, (((1,), (1,)), ((), ())), preferred_element_type=jnp.float32)
    back_up = lax.dot_general(up_grad, up_mat, (((1,), (1,)), ((), ())), preferred_element_type=jnp.float32)
    return back_gate + back_up


def reference(layer_input, out_grad, expert_ids, gate_probs, gate_proj, up_proj, down_proj):
    features = layer_input.shape[1]
    per_dev = TOK_DEV * TOP
    blocks = expert_ids.reshape(N_EP, per_dev).astype(jnp.int32)
    slot_rank = jax.vmap(lambda flat_ids: slot_ranks(flat_ids, EXPERTS))(blocks)
    source = jnp.arange(N_EP, dtype=jnp.int32)[:, None]
    token_index = source * TOK_DEV + jnp.arange(per_dev, dtype=jnp.int32)[None, :] // TOP
    column = (source * CAP + slot_rank).astype(jnp.int32)
    slot_token = jnp.full((EXPERTS, N_EP * CAP), TOKENS, jnp.int32).at[blocks, column].set(token_index.astype(jnp.int32))
    slot_prob = jnp.zeros((EXPERTS, N_EP * CAP), jnp.float32).at[blocks, column].set(gate_probs.reshape(N_EP, per_dev).astype(jnp.float32))
    padded_in = jnp.concatenate([layer_input, jnp.zeros((1, features), layer_input.dtype)], 0)
    padded_grad = jnp.concatenate([out_grad, jnp.zeros((1, features), out_grad.dtype)], 0)

    def per_expert(running_sum, expert_items):
        gate_mat, up_mat, down_mat, tokens_here, probs_here = expert_items
        result = expert_backward(padded_in[tokens_here], padded_grad[tokens_here], gate_mat, up_mat, down_mat).astype(jnp.bfloat16)
        running_sum = running_sum.at[tokens_here].add(result.astype(jnp.float32) * probs_here[:, None])
        return running_sum, None

    start_sum = jnp.zeros((TOKENS + 1, features), jnp.float32)
    running_sum, unused = lax.scan(per_expert, start_sum, (gate_proj, up_proj, down_proj, slot_token, slot_prob))
    return running_sum[:TOKENS].astype(jnp.bfloat16)
```

```python
import jax
import jax.numpy as jnp
from jax import lax
from jax.sharding import PartitionSpec as P


def body(layer_input, out_grad, expert_ids, gate_probs, gate_proj, up_proj, down_proj):
    experts = lax.axis_size("ep")
    halves = lax.axis_size("dp")
    tok_rows, features = layer_input.shape
    half = tok_rows // halves
    core = lax.axis_index("dp")
    start = core * half
    mine_in = lax.dynamic_slice_in_dim(layer_input, start, half, 0)
    mine_grad = lax.dynamic_slice_in_dim(out_grad, start, half, 0)
    ids = lax.dynamic_slice_in_dim(expert_ids, start, half, 0)
    probs = lax.dynamic_slice_in_dim(gate_probs, start, half, 0)
    names = jnp.arange(experts, dtype=jnp.int32)
    table = jnp.sum(
        jnp.where(ids[None, :, :] == names[:, None, None], probs[None, :, :], 0.0), axis=2
    )
    weight = lax.all_to_all(table, "ep", split_axis=0, concat_axis=0, tiled=True).reshape(-1)
    in_rows = lax.all_gather(mine_in, "ep", axis=0, tiled=True)
    grad_rows = lax.all_gather(mine_grad, "ep", axis=0, tiled=True)
    gate_mat, up_mat, down_mat = (gate_proj[0], up_proj[0], down_proj[0])
    nt = (((1,), (1,)), ((), ()))
    gate_pre = jnp.dot(in_rows, gate_mat, preferred_element_type=jnp.float32)
    up_pre = jnp.dot(in_rows, up_mat, preferred_element_type=jnp.float32)
    hidden_grad = lax.dot_general(grad_rows, down_mat, nt, preferred_element_type=jnp.float32)
    s = jax.nn.sigmoid(gate_pre)
    gate_grad = (hidden_grad * up_pre * s * (1.0 + gate_pre * (1.0 - s))).astype(jnp.bfloat16)
    up_grad = (hidden_grad * gate_pre * s).astype(jnp.bfloat16)
    back = lax.dot_general(gate_grad, gate_mat, nt, preferred_element_type=jnp.float32)
    back = back + lax.dot_general(up_grad, up_mat, nt, preferred_element_type=jnp.float32)
    back = (back * weight[:, None]).astype(jnp.bfloat16)
    mine = lax.psum_scatter(back, "ep", scatter_dimension=0, tiled=True)
    return lax.all_to_all(mine, "dp", split_axis=1, concat_axis=0, tiled=True)


def solution(mesh):
    row = P("ep", None)
    mat = P("ep", None, None)
    return jax.shard_map(
        body, mesh=mesh, in_specs=(row, row, row, row, mat, mat, mat), out_specs=P("ep", "dp"), check_vma=False
    )
```

```python
import functools

import jax
import jax.numpy as jnp
from jax import lax
from jax.experimental import pallas as pl
from jax.experimental.pallas import tpu as pltpu
from jax.sharding import PartitionSpec as P

MESH = pl.DeviceIdType.MESH
NT = (((1,), (1,)), ((), ()))


def flipped(z, j, planes):
    result, bit = z, 1
    while bit < planes:
        if j & bit:
            result = result + bit * (1 - 2 * ((z // bit) % 2))
        bit *= 2
    return result


def kernel(planes, x_hbm, g_hbm, w_ref, wg_hbm, wu_hbm, wd_hbm, out_ref,
           data, part, wgv, wuv, wdv, gg, ug, r1a, r1b, r2x, r2y, r3, fin,
           send_sem, recv_sem, load_sem):
    me, core = lax.axis_index("ep"), lax.axis_index("dp")
    z, y, x = me // 4, (me // 2) % 2, me % 2
    half, features = r2x.shape[1], r2x.shape[2]
    hidden = wgv.shape[1]
    cut = features // 2
    peer_x, peer_y = z * 4 + y * 2 + (1 - x), z * 4 + (1 - y) * 2 + x
    zs = [flipped(z, j, planes) for j in range(planes)]
    peer_z = [zs[j] * 4 + y * 2 + x for j in range(planes)]

    def block(j, dy, dx):
        by = (1 - y) if dy else y
        bx = (1 - x) if dx else x
        return pl.ds(pl.multiple_of((zs[j] * 4 + by * 2 + bx) * half, half), half)

    kinds = ("agz", "agx", "agy", "fa", "fb", "r1a", "r1b", "r2x", "r2y", "r3")
    sent = []

    def number(kind, j):
        return len(kinds) * planes if kind == "dp" else kinds.index(kind) * planes + j

    def send(kind, j, src, dst, to):
        n = number(kind, j)
        copy = pltpu.make_async_remote_copy(
            src_ref=src, dst_ref=dst, send_sem=send_sem.at[n], recv_sem=recv_sem.at[n],
            device_id=to, device_id_type=MESH,
        )
        copy.start()
        sent.append(copy)

    def arrive(kind, j, dst, to):
        n = number(kind, j)
        pltpu.make_async_remote_copy(
            src_ref=dst, dst_ref=dst, send_sem=send_sem.at[n], recv_sem=recv_sem.at[n],
            device_id=to, device_id_type=MESH,
        ).wait_recv()

    to_x, to_y, to_core = {"ep": peer_x}, {"ep": peer_y}, {"dp": 1 - core}
    own = block(0, 0, 0)
    mine = pl.ds(pl.multiple_of(core * half, half), half)
    first = [
        pltpu.make_async_copy(x_hbm.at[mine], data.at[0, own], load_sem.at[0]),
        pltpu.make_async_copy(g_hbm.at[mine], data.at[1, own], load_sem.at[1]),
    ]
    loads = [
        pltpu.make_async_copy(wg_hbm.at[0], wgv, load_sem.at[2]),
        pltpu.make_async_copy(wu_hbm.at[0], wuv, load_sem.at[3]),
        pltpu.make_async_copy(wd_hbm.at[0], wdv, load_sem.at[4]),
    ]
    for copy in first + loads:
        copy.start()

    barrier = pltpu.get_barrier_semaphore()
    greeted = [to_x, to_y, to_core] + [{"ep": peer_z[j]} for j in range(1, planes)]
    for other in greeted:
        pl.semaphore_signal(barrier, inc=1, device_id=other, device_id_type=MESH)
    pl.semaphore_wait(barrier, len(greeted))
    for copy in first:
        copy.wait()

    def gather(j):
        here = data.at[:, block(j, 0, 0), :]
        if j > 0:
            arrive("agz", j, here, {"ep": peer_z[j]})
        send("agx", j, here, here, to_x)
        send("agy", j, here, here, to_y)
        if j == 0:
            for i in range(1, planes):
                send("agz", i, here, here, {"ep": peer_z[i]})

    def forward(j):
        from_x = block(j, 0, 1)
        arrive("agx", j, data.at[:, from_x, :], to_x)
        piece = data.at[:, from_x, pl.ds(0, cut)]
        send("fa", j, piece, piece, to_y)
        from_y = block(j, 1, 0)
        arrive("agy", j, data.at[:, from_y, :], to_y)
        piece = data.at[:, from_y, pl.ds(cut, cut)]
        send("fb", j, piece, piece, to_x)

    def compute(j):
        far = block(j, 1, 1)
        arrive("fa", j, data.at[:, far, pl.ds(0, cut)], to_y)
        arrive("fb", j, data.at[:, far, pl.ds(cut, cut)], to_x)
        rows = pl.ds(pl.multiple_of(zs[j] * 4 * half, 4 * half), 4 * half)
        tile = 256

        @pl.loop(0, hidden // tile)
        def _(f):
            cols = pl.ds(pl.multiple_of(f * tile, tile), tile)
            tokens = data[0, rows, :]
            gate = jnp.dot(tokens, wgv[:, cols], preferred_element_type=jnp.float32)
            up = jnp.dot(tokens, wuv[:, cols], preferred_element_type=jnp.float32)
            grad = lax.dot_general(data[1, rows, :], wdv[cols, :], NT, preferred_element_type=jnp.float32)
            s = jax.nn.sigmoid(gate)
            gg[:, cols] = (grad * up * s * (1.0 + gate * (1.0 - s))).astype(jnp.bfloat16)
            ug[:, cols] = (grad * gate * s).astype(jnp.bfloat16)

        wide = 512

        @pl.loop(0, features // wide)
        def _(d):
            cols = pl.ds(pl.multiple_of(d * wide, wide), wide)
            back = lax.dot_general(gg[...], wgv[cols, :], NT, preferred_element_type=jnp.float32)
            back = back + lax.dot_general(ug[...], wuv[cols, :], NT, preferred_element_type=jnp.float32)
            part[rows, cols] = (back * w_ref[rows, :]).astype(jnp.bfloat16)

    def reduce1(j):
        far = block(j, 1, 1)
        send("r1a", j, part.at[far, pl.ds(0, cut)], r1a.at[j], to_y)
        send("r1b", j, part.at[far, pl.ds(cut, cut)], r1b.at[j], to_x)

    def reduce2(j):
        side = block(j, 0, 1)
        arrive("r1a", j, r1a.at[j], to_y)
        part[side, 0:cut] = (part[side, 0:cut].astype(jnp.float32) + r1a[j].astype(jnp.float32)).astype(jnp.bfloat16)
        send("r2x", j, part.at[side], r2x.at[j], to_x)
        side = block(j, 1, 0)
        arrive("r1b", j, r1b.at[j], to_x)
        part[side, cut:] = (part[side, cut:].astype(jnp.float32) + r1b[j].astype(jnp.float32)).astype(jnp.bfloat16)
        send("r2y", j, part.at[side], r2y.at[j], to_y)

    def reduce3(j):
        here = block(j, 0, 0)
        arrive("r2x", j, r2x.at[j], to_x)
        arrive("r2y", j, r2y.at[j], to_y)
        if j > 0:
            total = part[here, :].astype(jnp.float32) + r2x[j].astype(jnp.float32) + r2y[j].astype(jnp.float32)
            part[here, :] = total.astype(jnp.bfloat16)
            send("r3", j, part.at[here], r3.at[j], {"ep": peer_z[j]})

    steps = [(gather, 0), (forward, 0), (gather, 1)]
    for j in range(planes):
        if j == 0:
            for copy in loads:
                steps.append((lambda _, c=copy: c.wait(), 0))
        steps += [(compute, j), (reduce1, j)]
        if j + 1 < planes:
            steps.append((forward, j + 1))
        if j + 2 < planes:
            steps.append((gather, j + 2))
        if j >= 1:
            steps.append((reduce3, j - 1))
        steps.append((reduce2, j))
    steps.append((reduce3, planes - 1))
    for step, j in steps:
        step(j)

    for j in range(1, planes):
        arrive("r3", j, r3.at[j], {"ep": peer_z[j]})
    for h in range(2):
        cols = slice(h * cut, (h + 1) * cut)
        total = part[own, cols].astype(jnp.float32)
        total = total + r2x[0, :, cols].astype(jnp.float32) + r2y[0, :, cols].astype(jnp.float32)
        for j in range(1, planes):
            total = total + r3[j, :, cols].astype(jnp.float32)
        fin[h] = total.astype(jnp.bfloat16)
    keep = pltpu.make_async_copy(fin.at[core], out_ref.at[mine], load_sem.at[5])
    keep.start()
    send("dp", 0, fin.at[1 - core], out_ref.at[mine], to_core)
    theirs = pl.ds(pl.multiple_of((1 - core) * half, half), half)
    arrive("dp", 0, out_ref.at[theirs], to_core)
    keep.wait()
    for copy in sent:
        copy.wait_send()


def weights_of(expert_ids, gate_probs, experts, half, core):
    ids = lax.dynamic_slice_in_dim(expert_ids, core * half, half, 0)
    probs = lax.dynamic_slice_in_dim(gate_probs, core * half, half, 0)
    names = jnp.arange(experts, dtype=jnp.int32)
    table = jnp.sum(
        jnp.where(ids[None, :, :] == names[:, None, None], probs[None, :, :], 0.0), axis=2
    )
    return lax.all_to_all(table, "ep", split_axis=0, concat_axis=0, tiled=True).reshape(-1)


def fused(layer_input, out_grad, expert_ids, gate_probs, gate_proj, up_proj, down_proj):
    experts, halves = lax.axis_size("ep"), lax.axis_size("dp")
    tok_rows, features = layer_input.shape
    hidden = gate_proj.shape[2]
    half = tok_rows // halves
    planes = experts // 4
    weight = weights_of(expert_ids, gate_probs, experts, half, lax.axis_index("dp"))
    rows, cut, bf16 = experts * half, features // 2, jnp.bfloat16
    vmem, hbm = pl.BlockSpec(memory_space=pltpu.VMEM), pl.BlockSpec(memory_space=pl.ANY)
    count = 10 * planes + 1
    return pl.pallas_call(
        functools.partial(kernel, planes),
        name="fused_backward",
        out_shape=jax.ShapeDtypeStruct((tok_rows, features // halves), bf16),
        in_specs=[hbm, hbm, vmem, hbm, hbm, hbm],
        out_specs=vmem,
        scratch_shapes=[
            pltpu.VMEM((2, rows, features), bf16),
            pltpu.VMEM((rows, features), bf16),
            pltpu.VMEM((features, hidden), bf16),
            pltpu.VMEM((features, hidden), bf16),
            pltpu.VMEM((hidden, features), bf16),
            pltpu.VMEM((4 * half, hidden), bf16),
            pltpu.VMEM((4 * half, hidden), bf16),
            pltpu.VMEM((planes, half, cut), bf16),
            pltpu.VMEM((planes, half, cut), bf16),
            pltpu.VMEM((planes, half, features), bf16),
            pltpu.VMEM((planes, half, features), bf16),
            pltpu.VMEM((planes, half, features), bf16),
            pltpu.VMEM((halves, half, cut), bf16),
            pltpu.SemaphoreType.DMA((count,)),
            pltpu.SemaphoreType.DMA((count,)),
            pltpu.SemaphoreType.DMA((6,)),
        ],
        compiler_params=pltpu.CompilerParams(
            collective_id=0, has_side_effects=True, vmem_limit_bytes=67043328
        ),
    )(layer_input, out_grad, weight[:, None], gate_proj, up_proj, down_proj)


def dense(layer_input, out_grad, expert_ids, gate_probs, gate_proj, up_proj, down_proj):
    experts = lax.axis_size("ep")
    halves = lax.axis_size("dp")
    tok_rows, features = layer_input.shape
    half = tok_rows // halves
    core = lax.axis_index("dp")
    start = core * half
    mine_in = lax.dynamic_slice_in_dim(layer_input, start, half, 0)
    mine_grad = lax.dynamic_slice_in_dim(out_grad, start, half, 0)
    ids = lax.dynamic_slice_in_dim(expert_ids, start, half, 0)
    probs = lax.dynamic_slice_in_dim(gate_probs, start, half, 0)
    names = jnp.arange(experts, dtype=jnp.int32)
    table = jnp.sum(
        jnp.where(ids[None, :, :] == names[:, None, None], probs[None, :, :], 0.0), axis=2
    )
    weight = lax.all_to_all(table, "ep", split_axis=0, concat_axis=0, tiled=True).reshape(-1)
    in_rows = lax.all_gather(mine_in, "ep", axis=0, tiled=True)
    grad_rows = lax.all_gather(mine_grad, "ep", axis=0, tiled=True)
    gate_mat, up_mat, down_mat = (gate_proj[0], up_proj[0], down_proj[0])
    nt = (((1,), (1,)), ((), ()))
    gate_pre = jnp.dot(in_rows, gate_mat, preferred_element_type=jnp.float32)
    up_pre = jnp.dot(in_rows, up_mat, preferred_element_type=jnp.float32)
    hidden_grad = lax.dot_general(grad_rows, down_mat, nt, preferred_element_type=jnp.float32)
    s = jax.nn.sigmoid(gate_pre)
    gate_grad = (hidden_grad * up_pre * s * (1.0 + gate_pre * (1.0 - s))).astype(jnp.bfloat16)
    up_grad = (hidden_grad * gate_pre * s).astype(jnp.bfloat16)
    back = lax.dot_general(gate_grad, gate_mat, nt, preferred_element_type=jnp.float32)
    back = back + lax.dot_general(up_grad, up_mat, nt, preferred_element_type=jnp.float32)
    back = (back * weight[:, None]).astype(jnp.bfloat16)
    mine = lax.psum_scatter(back, "ep", scatter_dimension=0, tiled=True)
    return lax.all_to_all(mine, "dp", split_axis=1, concat_axis=0, tiled=True)


def body(*args):
    experts, halves = lax.axis_size("ep"), lax.axis_size("dp")
    tok_rows, features = args[0].shape
    hidden = args[4].shape[2]
    rows = experts * tok_rows // halves
    held = 2 * features * (3 * rows + 3 * hidden + rows)
    fits = held < 58 * 2**20 and halves == 2 and experts % 4 == 0
    return (fused if fits else dense)(*args)


def solution(mesh):
    row = P("ep", None)
    mat = P("ep", None, None)
    return jax.shard_map(
        body, mesh=mesh, in_specs=(row, row, row, row, mat, mat, mat), out_specs=P("ep", "dp"), check_vma=False
    )
```
